32 devices in a mesh: dp: 8 (over y, x, core), seq: 4 (over z).
Axes of the slice: x: 2, y: 2, z: 4, core: 2. Of those that a mesh axis runs over, the one named last changes fastest.
Arguments:
- img_q_raw: bfloat16 [8, 512, 1536], P('dp', 'seq'), may hold values from -12 to 12
- img_k_raw: bfloat16 [8, 512, 1536], P('dp', 'seq'), may hold values from -6 to 6
- img_v: bfloat16 [8, 512, 1536], P('dp', 'seq'), may hold values from -6 to 6
- img_dout: bfloat16 [8, 512, 1536], P('dp', 'seq'), may hold values from -6 to 6
- txt_q_raw: bfloat16 [8, 64, 1536], P('dp', 'seq'), may hold values from -6 to 6
- txt_k_raw: bfloat16 [8, 64, 1536], P('dp'), may hold values from -6 to 6
- txt_v: bfloat16 [8, 64, 1536], P('dp'), may hold values from -6 to 6
- txt_dout: bfloat16 [8, 64, 1536], P('dp', 'seq'), may hold values from -6 to 6
- q_gain: float32 [128], replicated, may hold values from 0.6 to 3.8
- k_gain: float32 [128], replicated, may hold values from 0.6 to 3.8
Outputs:
- img_dq: bfloat16 [8, 512, 1536], P('dp', 'seq')
- img_dk: bfloat16 [8, 512, 1536], P('dp', 'seq')
- img_dv: bfloat16 [8, 512, 1536], P('dp', 'seq')
- txt_dq: bfloat16 [8, 64, 1536], P('dp', 'seq')
- txt_dk: bfloat16 [8, 64, 1536], P('dp', 'seq')
- txt_dv: bfloat16 [8, 64, 1536], P('dp', 'seq')
- q_gain_grad: float32 [128], replicated
- k_gain_grad: float32 [128], replicated
The draws below stay inside these ranges and needn't reach their ends.
All inputs are finite; a program needn't handle non-finite values.
Results may differ from the reference program's by a relative error of at most 0.012.
The reference program's roundings to bfloat16 on the way count: a program that leaves them out, or rounds other values in their place, can miss the bound.
Values may be sent and summed in bfloat16 or wider, within the bound.
No kernel may reach another device: no remote copies, remote signals or barrier semaphores. Data moves between devices by JAX's collectives and lax.ppermute only.
A program may use at most 64 MiB of HBM per device.

```python
import jax
import jax.numpy as jnp
from jax import lax

HEADS = 12
HEAD_DIM = 128
IMG_DEV = 128
TEXT = 64
IMAGE = 512
BATCH = 8
N_SEQ = 4


def joint_image(key):
    base = jax.random.fold_in(key, 7)
    first_key, second_key = jax.random.split(base, 2)
    keys_image = jnp.clip(jax.random.normal(first_key, (BATCH, IMAGE, HEADS * HEAD_DIM), jnp.float32), -6.0, 6.0)
    queries = jnp.clip(jax.random.normal(second_key, (BATCH, IMAGE, HEADS * HEAD_DIM), jnp.float32), -6.0, 6.0)
    return (queries, keys_image)


def draw_img_q_raw(key, part):
    return joint_image(key)[0].astype(jnp.bfloat16)


def draw_img_k_raw(key, part):
    return joint_image(key)[1].astype(jnp.bfloat16)


def draw_q_gain(key, part):
    base = jax.random.fold_in(key, 11)
    return jax.random.uniform(base, (HEAD_DIM,), jnp.float32, 0.6, 1.4)


def draw_k_gain(key, part):
    base = jax.random.fold_in(key, 13)
    return jax.random.uniform(base, (HEAD_DIM,), jnp.float32, 0.6, 1.4)


def steps_of(key, shape, pieces, least, high):
    def one(dim, parts):
        heights = jax.random.uniform(jax.random.fold_in(jax.random.fold_in(key, 6), dim), (parts,), jnp.float32, least / len(pieces), high / len(pieces))
        return jnp.repeat(jnp.exp(heights), shape[dim] // parts).reshape((-1,) + (1,) * (len(shape) - dim - 1))

    factor_of = one(*pieces[0])
    for cut in pieces[1:]:
        factor_of = factor_of * one(*cut)
    return factor_of


def gaussian(key, extent, deviation, most, cuts=(), dtype=jnp.bfloat16):
    factor_of = steps_of(key, extent, cuts, -0.22, 0.18) if cuts else 1.0
    array = jax.random.normal(key, extent, jnp.float32) * deviation * factor_of
    return jnp.minimum(jnp.maximum(array, -most), most).astype(dtype)


def setup_inputs(seed: int = 0) -> dict:
    splits = jax.random.split(jax.random.key(seed), 11)
    return {
        "img_q_raw": draw_img_q_raw(jax.random.fold_in(splits[10], 71), 0),
        "img_k_raw": draw_img_k_raw(jax.random.fold_in(splits[10], 71), 0),
        "img_v": gaussian(splits[2], (BATCH, IMAGE, HEADS * HEAD_DIM), 1.0, 6.0, ((0, 8), (1, 4))),
        "img_dout": gaussian(splits[3], (BATCH, IMAGE, HEADS * HEAD_DIM), 1.0, 6.0, ((0, 8), (1, 4))),
        "txt_q_raw": gaussian(splits[4], (BATCH, TEXT, HEADS * HEAD_DIM), 1.0, 6.0, ((0, 8), (1, 4))),
        "txt_k_raw": gaussian(splits[5], (BATCH, TEXT, HEADS * HEAD_DIM), 1.0, 6.0, ((0, 8),)),
        "txt_v": gaussian(splits[6], (BATCH, TEXT, HEADS * HEAD_DIM), 1.0, 6.0, ((0, 8),)),
        "txt_dout": gaussian(splits[7], (BATCH, TEXT, HEADS * HEAD_DIM), 1.0, 6.0, ((0, 8), (1, 4))),
        "q_gain": draw_q_gain(jax.random.fold_in(splits[10], 71), 0),
        "k_gain": draw_k_gain(jax.random.fold_in(splits[10], 71), 0),
    }


epsilon = 1e-06

def normalize(source, norm_gain):
    values = source.astype(jnp.float32)
    inverse = lax.rsqrt(lax.optimization_barrier(jnp.mean(values * values, axis=-1, keepdims=True)) + epsilon)
    return values * inverse * norm_gain

def rounded(values):
    return lax.optimization_barrier(values.astype(jnp.bfloat16)).astype(jnp.float32)

def blocked(image_rows, text_rows):
    image_part = image_rows.reshape(N_SEQ, IMG_DEV, HEADS, HEAD_DIM)
    text_part = text_rows.reshape(N_SEQ, TEXT // N_SEQ, HEADS, HEAD_DIM)
    return jnp.concatenate([image_part, text_part], axis=1)

def sample(q_gain, k_gain, inputs):
    img_q, img_k, img_val, img_grad, txt_q, txt_k, txt_val, txt_grad = inputs
    query_src = blocked(img_q, txt_q).astype(jnp.float32)
    dout_f = blocked(img_grad, txt_grad).astype(jnp.float32)
    key_src = jnp.concatenate([img_k, txt_k], axis=0).reshape(IMAGE + TEXT, HEADS, HEAD_DIM).astype(jnp.float32)
    value_all = jnp.concatenate([img_val, txt_val], axis=0).reshape(IMAGE + TEXT, HEADS, HEAD_DIM).astype(jnp.float32)
    query_b = rounded(normalize(query_src, q_gain))
    key_b = rounded(normalize(key_src, k_gain))
    score_scale = HEAD_DIM ** (-0.5)
    scores = jnp.einsum('nqhd,khd->nhqk', query_b, key_b) * score_scale
    row_max = lax.optimization_barrier(jnp.max(scores, axis=-1, keepdims=True))
    shifted = scores - row_max
    log_total = jnp.log(lax.optimization_barrier(jnp.sum(jnp.exp(shifted), axis=-1, keepdims=True)))
    prob_full = jnp.exp(shifted - log_total)
    probs_b = rounded(prob_full)
    output_b = rounded(jnp.einsum('nhqk,khd->nqhd', probs_b, value_all))
    dprob = jnp.einsum('nqhd,khd->nhqk', dout_f, value_all)
    row_delta = jnp.transpose(lax.optimization_barrier(jnp.sum(dout_f * output_b, axis=-1)), (0, 2, 1))[..., None]
    dscore_b = rounded(prob_full * (dprob - row_delta) * score_scale)
    dquery = jnp.einsum('nhqk,khd->nqhd', dscore_b, key_b)
    dkey = lax.optimization_barrier(jnp.sum(rounded(jnp.einsum('nhqk,nqhd->nkhd', dscore_b, query_b)), axis=0))
    dvalue = lax.optimization_barrier(jnp.sum(rounded(jnp.einsum('nhqk,nqhd->nkhd', probs_b, dout_f)), axis=0))
    result_q, query_pull = jax.vjp(normalize, query_src, q_gain)
    dquery_src, dq_gain = query_pull(dquery)
    result_k, key_pull = jax.vjp(normalize, key_src, k_gain)
    dkey_src, dk_gain = key_pull(dkey)
    width_all = HEADS * HEAD_DIM
    dq_b = dquery_src.astype(jnp.bfloat16)
    image_dq = dq_b[:, :IMG_DEV].reshape(IMAGE, width_all)
    text_dq = dq_b[:, IMG_DEV:].reshape(TEXT, width_all)
    dk_b = dkey_src.reshape(IMAGE + TEXT, width_all).astype(jnp.bfloat16)
    dv_b = dvalue.reshape(IMAGE + TEXT, width_all).astype(jnp.bfloat16)
    return (image_dq, dk_b[:IMAGE], dv_b[:IMAGE], text_dq, dk_b[IMAGE:], dv_b[IMAGE:], dq_gain, dk_gain)

def reference(img_q_raw, img_k_raw, img_v, img_dout, txt_q_raw, txt_k_raw, txt_v, txt_dout, q_gain, k_gain):

    def per_sample(inputs):
        return sample(q_gain, k_gain, inputs)
    results = lax.map(per_sample, (img_q_raw, img_k_raw, img_v, img_dout, txt_q_raw, txt_k_raw, txt_v, txt_dout))
    return (results[0], results[1], results[2], results[3], results[4], results[5], lax.optimization_barrier(jnp.sum(results[6], axis=0)), lax.optimization_barrier(jnp.sum(results[7], axis=0)))
```

```python
import functools

import jax
import jax.numpy as jnp
from jax import lax
from jax.experimental import pallas as pl
from jax.experimental.pallas import tpu as pltpu
from jax.sharding import PartitionSpec as P

HEAD_DIM = 128
EPS = 1e-06


F32 = jnp.float32
BF16 = jnp.bfloat16


def pack_body(rows, trows, seq, pos_ref, *refs):
    ins, outs = refs[: 6 * seq], refs[6 * seq :]
    qn = rows + trows
    for r in range(seq):
        q, tq, d, td, k, v = ins[6 * r : 6 * r + 6]
        o = outs[r]
        o[0:rows] = q[...]
        o[rows:qn] = tq[...]
        o[qn : qn + rows] = d[...]
        o[qn + rows : 2 * qn] = td[...]
        o[2 * qn : 2 * qn + rows] = k[...]
        o[2 * qn + rows : 2 * qn + 2 * rows] = v[...]


def pack(pos, arrays, head, heads_here, seq):
    rows, trows = arrays[0].shape[0], arrays[1].shape[0]
    total = 4 * rows + 2 * trows

    def spec(r, n):
        return pl.BlockSpec(
            (n, HEAD_DIM), lambda i, p: (0, lax.rem(p[0] + r, seq) * heads_here + head)
        )

    in_specs, operands = [], []
    for r in range(seq):
        for a in arrays:
            in_specs.append(spec(r, a.shape[0]))
            operands.append(a)
    return pl.pallas_call(
        functools.partial(pack_body, rows, trows, seq),
        grid_spec=pltpu.PrefetchScalarGridSpec(
            num_scalar_prefetch=1,
            grid=(1,),
            in_specs=in_specs,
            out_specs=[pl.BlockSpec((total, HEAD_DIM), lambda i, p: (0, 0))] * seq,
        ),
        out_shape=[jax.ShapeDtypeStruct((total, HEAD_DIM), BF16)] * seq,
        name=f"pack{head}",
    )(pos, *operands)


def inverse_of(x):
    return lax.rsqrt(jnp.mean(x * x, axis=-1, keepdims=True) + EPS)


def norm_back(x, inv, g, up):
    xhat = x * inv
    gu = g * up
    dx = inv * (gu - xhat * jnp.mean(gu * xhat, axis=-1, keepdims=True))
    return dx, jnp.sum(up * xhat, axis=0, keepdims=True)


def dot(a, b, dims):
    return lax.dot_general(a, b, (dims, ((), ())), preferred_element_type=F32)


def attn_body(rows, trows, seq, pos_ref, *refs):
    parts = refs[:seq]
    tk, tv, qg, kg, gin = refs[seq : seq + 5]
    outs = refs[seq + 5 : 2 * seq + 5]
    gout = refs[2 * seq + 5]
    kn, vs, dka, dva = refs[2 * seq + 6 :]
    qn_rows = rows + trows
    img = rows * seq
    text = trows * seq
    scale = HEAD_DIM ** (-0.5)
    gq = qg[...]
    gk = kg[...]
    k0, v0 = 2 * qn_rows, 2 * qn_rows + rows
    for r in range(seq):
        x = parts[r][k0 : k0 + rows].astype(F32)
        kn[r * rows : (r + 1) * rows] = (x * inverse_of(x) * gk).astype(BF16)
        vs[r * rows : (r + 1) * rows] = parts[r][v0 : v0 + rows]
    xt = tk[...].astype(F32)
    kn[img : img + text] = (xt * inverse_of(xt) * gk).astype(BF16)
    vs[img : img + text] = tv[...]
    dq_gain = gin[0:1]
    dk_gain = gin[1:2]
    for r in range(seq):
        x = parts[r][0:qn_rows].astype(F32)
        inv = inverse_of(x)
        qb = (x * inv * gq).astype(BF16)
        d = parts[r][qn_rows : 2 * qn_rows]
        key = kn[...]
        val = vs[...]
        s = dot(qb, key, ((1,), (1,))) * scale
        e = jnp.exp(s - jnp.max(s, axis=-1, keepdims=True))
        prob = e * (1.0 / jnp.sum(e, axis=-1, keepdims=True))
        pb = prob.astype(BF16)
        out = dot(pb, val, ((1,), (0,))).astype(BF16).astype(F32)
        delta = jnp.sum(d.astype(F32) * out, axis=-1, keepdims=True)
        dp = dot(d, val, ((1,), (1,)))
        ds = (prob * (dp - delta) * scale).astype(BF16)
        dq = dot(ds, key, ((1,), (0,)))
        kp = dot(ds, qb, ((0,), (0,))).astype(BF16).astype(F32)
        vp = dot(pb, d, ((0,), (0,))).astype(BF16).astype(F32)
        if r == 0:
            dka[...] = kp
            dva[...] = vp
        else:
            dka[...] += kp
            dva[...] += vp
        dx, dg = norm_back(x, inv, gq, dq)
        dq_gain = dq_gain + dg
        outs[r][0:qn_rows] = dx.astype(BF16)
    for r in range(seq):
        x = parts[r][k0 : k0 + rows].astype(F32)
        dx, dg = norm_back(x, inverse_of(x), gk, dka[r * rows : (r + 1) * rows])
        dk_gain = dk_gain + dg
        outs[r][qn_rows : qn_rows + rows] = dx.astype(BF16)
        o = qn_rows + rows + trows
        outs[r][o : o + rows] = dva[r * rows : (r + 1) * rows].astype(BF16)
    dx, dg = norm_back(xt, inverse_of(xt), gk, dka[img : img + text])
    dk_gain = dk_gain + dg
    dka[img : img + text] = dx
    for r in range(seq):
        owner = lax.rem(pos_ref[0] + (seq - r), seq)
        at = pl.multiple_of(img + owner * trows, 16)
        o = qn_rows + rows
        outs[r][o : o + trows] = dka[pl.ds(at, trows)].astype(BF16)
        o = o + trows + rows
        outs[r][o : o + trows] = dva[pl.ds(at, trows)].astype(BF16)
    gout[0:1] = dq_gain
    gout[1:2] = dk_gain


def attend(pos, parts, text_k, text_v, q_gain, k_gain, gin, head, heads_here, rows, trows):
    seq = len(parts)
    keys = (rows + trows) * seq
    back = 3 * (rows + trows)

    def whole(shape):
        return pl.BlockSpec(shape, lambda i, p: (0,) * len(shape))

    tspec = pl.BlockSpec((text_k.shape[0], HEAD_DIM), lambda i, p: (0, p[0] * heads_here + head))
    return pl.pallas_call(
        functools.partial(attn_body, rows, trows, seq),
        grid_spec=pltpu.PrefetchScalarGridSpec(
            num_scalar_prefetch=1,
            grid=(1,),
            in_specs=[whole(p.shape) for p in parts]
            + [tspec, tspec, whole((1, HEAD_DIM)), whole((1, HEAD_DIM)), whole((2, HEAD_DIM))],
            out_specs=[whole((back, HEAD_DIM))] * seq + [whole((2, HEAD_DIM))],
            scratch_shapes=[
                pltpu.VMEM((keys, HEAD_DIM), BF16),
                pltpu.VMEM((keys, HEAD_DIM), BF16),
                pltpu.VMEM((keys, HEAD_DIM), F32),
                pltpu.VMEM((keys, HEAD_DIM), F32),
            ],
        ),
        out_shape=[jax.ShapeDtypeStruct((back, HEAD_DIM), BF16)] * seq
        + [jax.ShapeDtypeStruct((2, HEAD_DIM), F32)],
        name=f"attend{head}",
    )(pos, *parts, text_k, text_v, q_gain, k_gain, gin)


def unpack_body(rows, trows, seq, heads_here, pos_ref, *refs):
    n = seq * heads_here
    parts, outs = refs[:n], refs[n:]
    starts = (0, rows + trows, 2 * (rows + trows))
    for h in range(heads_here):
        for r in range(seq):
            p = parts[h * seq + r]
            col = (lax.rem(pos_ref[0] + r, seq) * heads_here + h) * HEAD_DIM
            lanes = pl.ds(pl.multiple_of(col, HEAD_DIM), HEAD_DIM)
            for j, at in enumerate(starts):
                outs[j][:, lanes] = p[at : at + rows]
                outs[3 + j][:, lanes] = p[at + rows : at + rows + trows]


def unpack(pos, parts, heads_here, seq, rows, trows):
    width = seq * heads_here * HEAD_DIM

    def whole(shape):
        return pl.BlockSpec(shape, lambda i, p: (0,) * len(shape))

    shapes = [(rows, width)] * 3 + [(trows, width)] * 3
    return pl.pallas_call(
        functools.partial(unpack_body, rows, trows, seq, heads_here),
        grid_spec=pltpu.PrefetchScalarGridSpec(
            num_scalar_prefetch=1,
            grid=(1,),
            in_specs=[whole(p.shape) for p in parts],
            out_specs=[whole(s) for s in shapes],
        ),
        out_shape=[jax.ShapeDtypeStruct(s, BF16) for s in shapes],
        name="unpack",
    )(pos, *parts)


def factors_of(n):
    found, f = [], 2
    while n > 1:
        while n % f == 0:
            found.append(f)
            n //= f
        f += 1
    return found


def sum_over(x, axis):
    size = lax.axis_size(axis)
    index = lax.axis_index(axis)
    stride = 1
    for f in factors_of(size):
        digit = lax.rem(index // stride, f)

        def moved(i, k):
            dg = (i // stride) % f
            return i + ((dg + k) % f - dg) * stride

        got = [x]
        for k in range(1, f):
            got.append(lax.ppermute(x, axis, [(i, moved(i, k)) for i in range(size)]))
        if f == 2:
            x = got[0] + got[1]
        else:
            stack = jnp.stack(got)
            x = 0.0
            for j in range(f):
                x = x + lax.dynamic_index_in_dim(stack, lax.rem(digit - j + f, f), 0, False)
        stride *= f
    return x


def rotate(x, r, seq):
    return lax.ppermute(x, "seq", [(i, (i + r) % seq) for i in range(seq)])


def local(
    img_q_raw, img_k_raw, img_v, img_dout, txt_q_raw, txt_k_raw, txt_v, txt_dout, q_gain, k_gain
):
    seq = lax.axis_size("seq")
    pos = lax.axis_index("seq").astype(jnp.int32).reshape(1)
    rows, width = img_q_raw.shape[1:]
    trows = txt_q_raw.shape[1]
    heads_here = width // HEAD_DIM // seq
    arrays = (img_q_raw[0], txt_q_raw[0], img_dout[0], txt_dout[0], img_k_raw[0], img_v[0])
    text_k, text_v = txt_k_raw[0], txt_v[0]
    gq, gk = q_gain.reshape(1, HEAD_DIM), k_gain.reshape(1, HEAD_DIM)
    received = []
    for h in range(heads_here):
        sent = pack(pos, arrays, h, heads_here, seq)
        received.append([sent[0]] + [rotate(sent[r], r, seq) for r in range(1, seq)])
    gains = jnp.zeros((2, HEAD_DIM), F32)
    back = []
    for h in range(heads_here):
        *outs, gains = attend(
            pos, received[h], text_k, text_v, gq, gk, gains, h, heads_here, rows, trows
        )
        back += [outs[0]] + [rotate(outs[r], seq - r, seq) for r in range(1, seq)]
    gains = sum_over(sum_over(gains, "dp"), "seq")
    grads = unpack(pos, back, heads_here, seq, rows, trows)
    return tuple(g[None] for g in grads) + (gains[0], gains[1])


def solution(mesh):
    token = P("dp", "seq", None)
    shared = P("dp", None, None)
    return jax.shard_map(
        local,
        mesh=mesh,
        in_specs=(token, token, token, token, token, shared, shared, token, P(), P()),
        out_specs=(token,) * 6 + (P(), P()),
        check_vma=False,
    )
```

```python
import functools

import jax
import jax.numpy as jnp
from jax import lax
from jax.experimental import pallas as pl
from jax.experimental.pallas import tpu as pltpu
from jax.sharding import PartitionSpec as P


HEAD_DIM = 128
EPS = 1e-06


F32 = jnp.float32
BF16 = jnp.bfloat16


def copies(pairs, sems):
    started = [pltpu.make_async_copy(src, dst, sems.at[i]) for i, (src, dst) in enumerate(pairs)]
    for c in started:
        c.start()
    for c in started:
        c.wait()


def lanes_of(pos_ref, r, seq, heads_here, head):
    col = (lax.rem(pos_ref[0] + r, seq) * heads_here + head) * HEAD_DIM
    return pl.ds(pl.multiple_of(col, HEAD_DIM), HEAD_DIM)


def pack_body(seq, heads_here, head, pos_ref, *refs):
    ins, outs, sems = refs[:6], refs[6 : 6 + seq], refs[6 + seq]
    pairs = []
    for j in range(1, seq + 1):
        r = j % seq
        lanes = lanes_of(pos_ref, r, seq, heads_here, head)
        at = 0
        for a in ins:
            n = a.shape[0]
            pairs.append((a.at[:, lanes], outs[r].at[pl.ds(at, n)]))
            at += n
    copies(pairs, sems)


def pack(pos, arrays, head, heads_here, seq):
    total = sum(a.shape[0] for a in arrays)
    anywhere = pl.BlockSpec(memory_space=pl.ANY)
    return pl.pallas_call(
        functools.partial(pack_body, seq, heads_here, head),
        in_specs=[pl.BlockSpec(memory_space=pltpu.SMEM)] + [anywhere] * len(arrays),
        out_specs=[anywhere] * seq,
        out_shape=[jax.ShapeDtypeStruct((total, HEAD_DIM), BF16)] * seq,
        scratch_shapes=[pltpu.SemaphoreType.DMA((seq * len(arrays),))],
    )(pos, *arrays)


def inverse_of(x):
    return lax.rsqrt(jnp.mean(x * x, axis=-1, keepdims=True) + EPS)


def norm_back(x, inv, g, up):
    xhat = x * inv
    gu = g * up
    dx = inv * (gu - xhat * jnp.mean(gu * xhat, axis=-1, keepdims=True))
    return dx, jnp.sum(up * xhat, axis=0, keepdims=True)


def dot(a, b, dims):
    return lax.dot_general(a, b, (dims, ((), ())), preferred_element_type=F32)


def attn_body(rows, trows, seq, pos_ref, *refs):
    parts = refs[:seq]
    tk, tv, qg, kg, gin = refs[seq : seq + 5]
    outs = refs[seq + 5 : 2 * seq + 5]
    gout = refs[2 * seq + 5]
    kn, vs, dka, dva = refs[2 * seq + 6 :]
    qn_rows = rows + trows
    img = rows * seq
    text = trows * seq
    scale = HEAD_DIM ** (-0.5)
    gq = qg[...]
    gk = kg[...]
    k0, v0 = 2 * qn_rows, 2 * qn_rows + rows
    for r in range(seq):
        x = parts[r][k0 : k0 + rows].astype(F32)
        kn[r * rows : (r + 1) * rows] = (x * inverse_of(x) * gk).astype(BF16)
        vs[r * rows : (r + 1) * rows] = parts[r][v0 : v0 + rows]
    xt = tk[...].astype(F32)
    kn[img : img + text] = (xt * inverse_of(xt) * gk).astype(BF16)
    vs[img : img + text] = tv[...]
    dq_gain = gin[0:1]
    dk_gain = gin[1:2]
    for r in range(seq):
        x = parts[r][0:qn_rows].astype(F32)
        inv = inverse_of(x)
        qb = (x * inv * gq).astype(BF16)
        d = parts[r][qn_rows : 2 * qn_rows]
        key = kn[...]
        val = vs[...]
        s = dot(qb, key, ((1,), (1,))) * scale
        e = jnp.exp(s - jnp.max(s, axis=-1, keepdims=True))
        prob = e * (1.0 / jnp.sum(e, axis=-1, keepdims=True))
        pb = prob.astype(BF16)
        out = dot(pb, val, ((1,), (0,))).astype(BF16).astype(F32)
        delta = jnp.sum(d.astype(F32) * out, axis=-1, keepdims=True)
        dp = dot(d, val, ((1,), (1,)))
        ds = (prob * (dp - delta) * scale).astype(BF16)
        dq = dot(ds, key, ((1,), (0,)))
        kp = dot(ds, qb, ((0,), (0,))).astype(BF16).astype(F32)
        vp = dot(pb, d, ((0,), (0,))).astype(BF16).astype(F32)
        if r == 0:
            dka[...] = kp
            dva[...] = vp
        else:
            dka[...] += kp
            dva[...] += vp
        dx, dg = norm_back(x, inv, gq, dq)
        dq_gain = dq_gain + dg
        outs[r][0:qn_rows] = dx.astype(BF16)
    for r in range(seq):
        x = parts[r][k0 : k0 + rows].astype(F32)
        dx, dg = norm_back(x, inverse_of(x), gk, dka[r * rows : (r + 1) * rows])
        dk_gain = dk_gain + dg
        outs[r][qn_rows : qn_rows + rows] = dx.astype(BF16)
        o = qn_rows + rows + trows
        outs[r][o : o + rows] = dva[r * rows : (r + 1) * rows].astype(BF16)
    dx, dg = norm_back(xt, inverse_of(xt), gk, dka[img : img + text])
    dk_gain = dk_gain + dg
    dka[img : img + text] = dx
    for r in range(seq):
        owner = lax.rem(pos_ref[0] + (seq - r), seq)
        at = pl.multiple_of(img + owner * trows, 16)
        o = qn_rows + rows
        outs[r][o : o + trows] = dka[pl.ds(at, trows)].astype(BF16)
        o = o + trows + rows
        outs[r][o : o + trows] = dva[pl.ds(at, trows)].astype(BF16)
    gout[0:1] = dq_gain
    gout[1:2] = dk_gain


def attend(pos, parts, text_k, text_v, q_gain, k_gain, gin, head, heads_here, rows, trows):
    seq = len(parts)
    keys = (rows + trows) * seq
    back = 3 * (rows + trows)

    def whole(shape):
        return pl.BlockSpec(shape, lambda i, p: (0,) * len(shape))

    tspec = pl.BlockSpec((text_k.shape[0], HEAD_DIM), lambda i, p: (0, p[0] * heads_here + head))
    return pl.pallas_call(
        functools.partial(attn_body, rows, trows, seq),
        grid_spec=pltpu.PrefetchScalarGridSpec(
            num_scalar_prefetch=1,
            grid=(1,),
            in_specs=[whole(p.shape) for p in parts]
            + [tspec, tspec, whole((1, HEAD_DIM)), whole((1, HEAD_DIM)), whole((2, HEAD_DIM))],
            out_specs=[whole((back, HEAD_DIM))] * seq + [whole((2, HEAD_DIM))],
            scratch_shapes=[
                pltpu.VMEM((keys, HEAD_DIM), BF16),
                pltpu.VMEM((keys, HEAD_DIM), BF16),
                pltpu.VMEM((keys, HEAD_DIM), F32),
                pltpu.VMEM((keys, HEAD_DIM), F32),
            ],
        ),
        out_shape=[jax.ShapeDtypeStruct((back, HEAD_DIM), BF16)] * seq
        + [jax.ShapeDtypeStruct((2, HEAD_DIM), F32)],
    )(pos, *parts, text_k, text_v, q_gain, k_gain, gin)


def unpack_body(rows, trows, seq, heads_here, head, pos_ref, *refs):
    parts, outs, sems = refs[:seq], refs[-7:-1], refs[-1]
    pairs = []
    for r in range(seq):
        lanes = lanes_of(pos_ref, r, seq, heads_here, head)
        for j in range(3):
            at = j * (rows + trows)
            pairs.append((parts[r].at[pl.ds(at, rows)], outs[j].at[:, lanes]))
            pairs.append((parts[r].at[pl.ds(at + rows, trows)], outs[3 + j].at[:, lanes]))
    copies(pairs, sems)


def unpack(pos, parts, grads, head, heads_here, rows, trows):
    seq = len(parts)
    width = seq * heads_here * HEAD_DIM
    anywhere = pl.BlockSpec(memory_space=pl.ANY)
    shapes = [(rows, width)] * 3 + [(trows, width)] * 3
    return pl.pallas_call(
        functools.partial(unpack_body, rows, trows, seq, heads_here, head),
        in_specs=[pl.BlockSpec(memory_space=pltpu.SMEM)] + [anywhere] * (seq + len(grads)),
        out_specs=[anywhere] * 6,
        out_shape=[jax.ShapeDtypeStruct(s, BF16) for s in shapes],
        input_output_aliases={1 + seq + i: i for i in range(len(grads))},
        scratch_shapes=[pltpu.SemaphoreType.DMA((6 * seq,))],
    )(pos, *parts, *grads)


def factors_of(n):
    found, f = [], 2
    while n > 1:
        while n % f == 0:
            found.append(f)
            n //= f
        f += 1
    return found


def sum_over(x, axis, factors):
    size = lax.axis_size(axis)
    index = lax.axis_index(axis)
    stride = 1
    for f in factors:
        digit = lax.rem(index // stride, f)

        def moved(i, k):
            dg = (i // stride) % f
            return i + ((dg + k) % f - dg) * stride

        got = [x]
        for k in range(1, f):
            got.append(lax.ppermute(x, axis, [(i, moved(i, k)) for i in range(size)]))
        if f == 2:
            x = got[0] + got[1]
        else:
            stack = jnp.stack(got)
            x = 0.0
            for j in range(f):
                x = x + lax.dynamic_index_in_dim(stack, lax.rem(digit - j + f, f), 0, False)
        stride *= f
    return x


def rotate(x, r, seq):
    return lax.ppermute(x, "seq", [(i, (i + r) % seq) for i in range(seq)])


def local(
    img_q_raw, img_k_raw, img_v, img_dout, txt_q_raw, txt_k_raw, txt_v, txt_dout, q_gain, k_gain
):
    seq = lax.axis_size("seq")
    pos = lax.axis_index("seq").astype(jnp.int32).reshape(1)
    rows, width = img_q_raw.shape[1:]
    trows = txt_q_raw.shape[1]
    heads_here = width // HEAD_DIM // seq
    arrays = (img_q_raw[0], txt_q_raw[0], img_dout[0], txt_dout[0], img_k_raw[0], img_v[0])
    text_k, text_v = txt_k_raw[0], txt_v[0]
    gq, gk = q_gain.reshape(1, HEAD_DIM), k_gain.reshape(1, HEAD_DIM)
    received = []
    for h in range(heads_here):
        sent = pack(pos, arrays, h, heads_here, seq)
        received.append([sent[0]] + [rotate(sent[r], r, seq) for r in range(1, seq)])
    gains = jnp.zeros((2, HEAD_DIM), F32)
    back = []
    for h in range(heads_here):
        *outs, gains = attend(
            pos, received[h], text_k, text_v, gq, gk, gains, h, heads_here, rows, trows
        )
        back.append([outs[0]] + [rotate(outs[r], seq - r, seq) for r in range(1, seq)])
    gains = sum_over(gains, "seq", [seq])
    gains = sum_over(gains, "dp", factors_of(lax.axis_size("dp")))
    grads = []
    for h in range(heads_here):
        grads = unpack(pos, back[h], grads, h, heads_here, rows, trows)
    return tuple(g[None] for g in grads) + (gains[0], gains[1])


def solution(mesh):
    token = P("dp", "seq", None)
    shared = P("dp", None, None)
    return jax.shard_map(
        local,
        mesh=mesh,
        in_specs=(token, token, token, token, token, shared, shared, token, P(), P()),
        out_specs=(token,) * 6 + (P(), P()),
        check_vma=False,
    )
```

```python
import functools

import jax
import jax.numpy as jnp
from jax import lax
from jax.experimental import pallas as pl
from jax.experimental.pallas import tpu as pltpu
from jax.sharding import PartitionSpec as P


HEAD_DIM = 128
EPS = 1e-06


F32 = jnp.float32
BF16 = jnp.bfloat16


def pack_body(rows, trows, seq, pos_ref, *refs):
    ins, outs = refs[: 6 * seq], refs[6 * seq :]
    qn = rows + trows
    for r in range(seq):
        q, tq, d, td, k, v = ins[6 * r : 6 * r + 6]
        o = outs[r]
        o[0:rows] = q[...]
        o[rows:qn] = tq[...]
        o[qn : qn + rows] = d[...]
        o[qn + rows : 2 * qn] = td[...]
        o[2 * qn : 2 * qn + rows] = k[...]
        o[2 * qn + rows : 2 * qn + 2 * rows] = v[...]


def pack(pos, arrays, head, heads_here, seq):
    rows, trows = arrays[0].shape[0], arrays[1].shape[0]
    total = 4 * rows + 2 * trows

    def spec(r, n):
        return pl.BlockSpec(
            (n, HEAD_DIM), lambda i, p: (0, lax.rem(p[0] + r, seq) * heads_here + head)
        )

    in_specs, operands = [], []
    for r in range(seq):
        for a in arrays:
            in_specs.append(spec(r, a.shape[0]))
            operands.append(a)
    return pl.pallas_call(
        functools.partial(pack_body, rows, trows, seq),
        grid_spec=pltpu.PrefetchScalarGridSpec(
            num_scalar_prefetch=1,
            grid=(1,),
            in_specs=in_specs,
            out_specs=[pl.BlockSpec((total, HEAD_DIM), lambda i, p: (0, 0))] * seq,
        ),
        out_shape=[jax.ShapeDtypeStruct((total, HEAD_DIM), BF16)] * seq,
    )(pos, *operands)


def inverse_of(x):
    return lax.rsqrt(jnp.mean(x * x, axis=-1, keepdims=True) + EPS)


def norm_back(x, inv, g, up):
    xhat = x * inv
    gu = g * up
    dx = inv * (gu - xhat * jnp.mean(gu * xhat, axis=-1, keepdims=True))
    return dx, jnp.sum(up * xhat, axis=0, keepdims=True)


def dot(a, b, dims):
    return lax.dot_general(a, b, (dims, ((), ())), preferred_element_type=F32)


def attn_body(rows, trows, seq, pos_ref, *refs):
    parts = refs[:seq]
    tk, tv, qg, kg, gin = refs[seq : seq + 5]
    outs = refs[seq + 5 : 2 * seq + 5]
    gout = refs[2 * seq + 5]
    kn, vs, dka, dva = refs[2 * seq + 6 :]
    qn_rows = rows + trows
    img = rows * seq
    text = trows * seq
    scale = HEAD_DIM ** (-0.5)
    gq = qg[...]
    gk = kg[...]
    k0, v0 = 2 * qn_rows, 2 * qn_rows + rows
    for r in range(seq):
        x = parts[r][k0 : k0 + rows].astype(F32)
        kn[r * rows : (r + 1) * rows] = (x * inverse_of(x) * gk).astype(BF16)
        vs[r * rows : (r + 1) * rows] = parts[r][v0 : v0 + rows]
    xt = tk[...].astype(F32)
    kn[img : img + text] = (xt * inverse_of(xt) * gk).astype(BF16)
    vs[img : img + text] = tv[...]
    dq_gain = gin[0:1]
    dk_gain = gin[1:2]
    for r in range(seq):
        x = parts[r][0:qn_rows].astype(F32)
        inv = inverse_of(x)
        qb = (x * inv * gq).astype(BF16)
        d = parts[r][qn_rows : 2 * qn_rows]
        key = kn[...]
        val = vs[...]
        s = dot(qb, key, ((1,), (1,))) * scale
        e = jnp.exp(s - jnp.max(s, axis=-1, keepdims=True))
        prob = e * (1.0 / jnp.sum(e, axis=-1, keepdims=True))
        pb = prob.astype(BF16)
        out = dot(pb, val, ((1,), (0,))).astype(BF16).astype(F32)
        delta = jnp.sum(d.astype(F32) * out, axis=-1, keepdims=True)
        dp = dot(d, val, ((1,), (1,)))
        ds = (prob * (dp - delta) * scale).astype(BF16)
        dq = dot(ds, key, ((1,), (0,)))
        kp = dot(ds, qb, ((0,), (0,))).astype(BF16).astype(F32)
        vp = dot(pb, d, ((0,), (0,))).astype(BF16).astype(F32)
        if r == 0:
            dka[...] = kp
            dva[...] = vp
        else:
            dka[...] += kp
            dva[...] += vp
        dx, dg = norm_back(x, inv, gq, dq)
        dq_gain = dq_gain + dg
        outs[r][0:qn_rows] = dx.astype(BF16)
    for r in range(seq):
        x = parts[r][k0 : k0 + rows].astype(F32)
        dx, dg = norm_back(x, inverse_of(x), gk, dka[r * rows : (r + 1) * rows])
        dk_gain = dk_gain + dg
        outs[r][qn_rows : qn_rows + rows] = dx.astype(BF16)
        o = qn_rows + rows + trows
        outs[r][o : o + rows] = dva[r * rows : (r + 1) * rows].astype(BF16)
    dx, dg = norm_back(xt, inverse_of(xt), gk, dka[img : img + text])
    dk_gain = dk_gain + dg
    dka[img : img + text] = dx
    for r in range(seq):
        owner = lax.rem(pos_ref[0] + (seq - r), seq)
        at = pl.multiple_of(img + owner * trows, 16)
        o = qn_rows + rows
        outs[r][o : o + trows] = dka[pl.ds(at, trows)].astype(BF16)
        o = o + trows + rows
        outs[r][o : o + trows] = dva[pl.ds(at, trows)].astype(BF16)
    gout[0:1] = dq_gain
    gout[1:2] = dk_gain


def attend(pos, parts, text_k, text_v, q_gain, k_gain, gin, head, heads_here, rows, trows):
    seq = len(parts)
    keys = (rows + trows) * seq
    back = 3 * (rows + trows)

    def whole(shape):
        return pl.BlockSpec(shape, lambda i, p: (0,) * len(shape))

    tspec = pl.BlockSpec((text_k.shape[0], HEAD_DIM), lambda i, p: (0, p[0] * heads_here + head))
    return pl.pallas_call(
        functools.partial(attn_body, rows, trows, seq),
        grid_spec=pltpu.PrefetchScalarGridSpec(
            num_scalar_prefetch=1,
            grid=(1,),
            in_specs=[whole(p.shape) for p in parts]
            + [tspec, tspec, whole((1, HEAD_DIM)), whole((1, HEAD_DIM)), whole((2, HEAD_DIM))],
            out_specs=[whole((back, HEAD_DIM))] * seq + [whole((2, HEAD_DIM))],
            scratch_shapes=[
                pltpu.VMEM((keys, HEAD_DIM), BF16),
                pltpu.VMEM((keys, HEAD_DIM), BF16),
                pltpu.VMEM((keys, HEAD_DIM), F32),
                pltpu.VMEM((keys, HEAD_DIM), F32),
            ],
        ),
        out_shape=[jax.ShapeDtypeStruct((back, HEAD_DIM), BF16)] * seq
        + [jax.ShapeDtypeStruct((2, HEAD_DIM), F32)],
    )(pos, *parts, text_k, text_v, q_gain, k_gain, gin)


def unpack_body(rows, trows, seq, pos_ref, *refs):
    parts, outs = refs[:seq], refs[-6:]
    for r in range(seq):

        @pl.when(pl.program_id(0) == r)
        def _():
            for j in range(3):
                at = j * (rows + trows)
                outs[j][...] = parts[r][at : at + rows]
                outs[3 + j][...] = parts[r][at + rows : at + rows + trows]


def unpack(pos, parts, grads, head, heads_here, rows, trows):
    seq = len(parts)
    width = seq * heads_here * HEAD_DIM

    def lanes(i, p):
        return (0, lax.rem(p[0] + i, seq) * heads_here + head)

    heights = [rows] * 3 + [trows] * 3
    return pl.pallas_call(
        functools.partial(unpack_body, rows, trows, seq),
        grid_spec=pltpu.PrefetchScalarGridSpec(
            num_scalar_prefetch=1,
            grid=(seq,),
            in_specs=[pl.BlockSpec(p.shape, lambda i, p: (0, 0)) for p in parts]
            + [pl.BlockSpec(memory_space=pl.ANY)] * len(grads),
            out_specs=[pl.BlockSpec((n, HEAD_DIM), lanes) for n in heights],
        ),
        out_shape=[jax.ShapeDtypeStruct((n, width), BF16) for n in heights],
        input_output_aliases={1 + seq + i: i for i in range(len(grads))},
    )(pos, *parts, *grads)


def factors_of(n):
    found, f = [], 2
    while n > 1:
        while n % f == 0:
            found.append(f)
            n //= f
        f += 1
    return found


def sum_over(x, axis, factors):
    size = lax.axis_size(axis)
    index = lax.axis_index(axis)
    stride = 1
    for f in factors:
        digit = lax.rem(index // stride, f)

        def moved(i, k):
            dg = (i // stride) % f
            return i + ((dg + k) % f - dg) * stride

        got = [x]
        for k in range(1, f):
            got.append(lax.ppermute(x, axis, [(i, moved(i, k)) for i in range(size)]))
        if f == 2:
            x = got[0] + got[1]
        else:
            stack = jnp.stack(got)
            x = 0.0
            for j in range(f):
                x = x + lax.dynamic_index_in_dim(stack, lax.rem(digit - j + f, f), 0, False)
        stride *= f
    return x


def rotate(x, r, seq):
    return lax.ppermute(x, "seq", [(i, (i + r) % seq) for i in range(seq)])


def local(
    img_q_raw, img_k_raw, img_v, img_dout, txt_q_raw, txt_k_raw, txt_v, txt_dout, q_gain, k_gain
):
    seq = lax.axis_size("seq")
    pos = lax.axis_index("seq").astype(jnp.int32).reshape(1)
    rows, width = img_q_raw.shape[1:]
    trows = txt_q_raw.shape[1]
    heads_here = width // HEAD_DIM // seq
    arrays = (img_q_raw[0], txt_q_raw[0], img_dout[0], txt_dout[0], img_k_raw[0], img_v[0])
    text_k, text_v = txt_k_raw[0], txt_v[0]
    gq, gk = q_gain.reshape(1, HEAD_DIM), k_gain.reshape(1, HEAD_DIM)
    received = []
    for h in range(heads_here):
        sent = pack(pos, arrays, h, heads_here, seq)
        received.append([sent[0]] + [rotate(sent[r], r, seq) for r in range(1, seq)])
    gains = jnp.zeros((2, HEAD_DIM), F32)
    back = []
    for h in range(heads_here):
        *outs, gains = attend(
            pos, received[h], text_k, text_v, gq, gk, gains, h, heads_here, rows, trows
        )
        back.append([outs[0]] + [rotate(outs[r], seq - r, seq) for r in range(1, seq)])
    gains = sum_over(gains, "seq", [seq])
    gains = sum_over(gains, "dp", factors_of(lax.axis_size("dp")))
    grads = []
    for h in range(heads_here):
        grads = unpack(pos, back[h], grads, h, heads_here, rows, trows)
    return tuple(g[None] for g in grads) + (gains[0], gains[1])


def solution(mesh):
    token = P("dp", "seq", None)
    shared = P("dp", None, None)
    return jax.shard_map(
        local,
        mesh=mesh,
        in_specs=(token, token, token, token, token, shared, shared, token, P(), P()),
        out_specs=(token,) * 6 + (P(), P()),
        check_vma=False,
    )
```

```python
import functools

import jax
import jax.numpy as jnp
from jax import lax
from jax.experimental import pallas as pl
from jax.experimental.pallas import tpu as pltpu
from jax.sharding import PartitionSpec as P


HEAD_DIM = 128
EPS = 1e-06


F32 = jnp.float32
BF16 = jnp.bfloat16


def pack_body(rows, trows, seq, pos_ref, *refs):
    ins, outs = refs[: 6 * seq], refs[6 * seq :]
    qn = rows + trows
    for r in range(seq):
        q, tq, d, td, k, v = ins[6 * r : 6 * r + 6]
        o = outs[r]
        o[0:rows] = q[...]
        o[rows:qn] = tq[...]
        o[qn : qn + rows] = d[...]
        o[qn + rows : 2 * qn] = td[...]
        o[2 * qn : 2 * qn + rows] = k[...]
        o[2 * qn + rows : 2 * qn + 2 * rows] = v[...]


def pack(pos, arrays, head, heads_here, seq):
    rows, trows = arrays[0].shape[0], arrays[1].shape[0]
    total = 4 * rows + 2 * trows

    def spec(r, n):
        return pl.BlockSpec(
            (n, HEAD_DIM), lambda i, p: (0, lax.rem(p[0] + r, seq) * heads_here + head)
        )

    in_specs, operands = [], []
    for r in range(seq):
        for a in arrays:
            in_specs.append(spec(r, a.shape[0]))
            operands.append(a)
    return pl.pallas_call(
        functools.partial(pack_body, rows, trows, seq),
        grid_spec=pltpu.PrefetchScalarGridSpec(
            num_scalar_prefetch=1,
            grid=(1,),
            in_specs=in_specs,
            out_specs=[pl.BlockSpec((total, HEAD_DIM), lambda i, p: (0, 0))] * seq,
        ),
        out_shape=[jax.ShapeDtypeStruct((total, HEAD_DIM), BF16)] * seq,
    )(pos, *operands)


def inverse_of(x):
    return lax.rsqrt(jnp.mean(x * x, axis=-1, keepdims=True) + EPS)


def norm_back(x, inv, g, up):
    xhat = x * inv
    gu = g * up
    dx = inv * (gu - xhat * jnp.mean(gu * xhat, axis=-1, keepdims=True))
    return dx, jnp.sum(up * xhat, axis=0, keepdims=True)


def dot(a, b, dims):
    return lax.dot_general(a, b, (dims, ((), ())), preferred_element_type=F32)


def attn_body(rows, trows, seq, pos_ref, *refs):
    parts = refs[:seq]
    tk, tv, qg, kg, gin = refs[seq : seq + 5]
    outs = refs[seq + 5 : 2 * seq + 5]
    gout = refs[2 * seq + 5]
    kn, vs, dka, dva = refs[2 * seq + 6 :]
    qn_rows = rows + trows
    img = rows * seq
    text = trows * seq
    scale = HEAD_DIM ** (-0.5)
    gq = qg[...]
    gk = kg[...]
    k0, v0 = 2 * qn_rows, 2 * qn_rows + rows
    for r in range(seq):
        x = parts[r][k0 : k0 + rows].astype(F32)
        kn[r * rows : (r + 1) * rows] = (x * inverse_of(x) * gk).astype(BF16)
        vs[r * rows : (r + 1) * rows] = parts[r][v0 : v0 + rows]
    xt = tk[...].astype(F32)
    kn[img : img + text] = (xt * inverse_of(xt) * gk).astype(BF16)
    vs[img : img + text] = tv[...]
    dq_gain = gin[0:1]
    dk_gain = gin[1:2]
    for r in range(seq):
        x = parts[r][0:qn_rows].astype(F32)
        inv = inverse_of(x)
        qb = (x * inv * gq).astype(BF16)
        d = parts[r][qn_rows : 2 * qn_rows]
        key = kn[...]
        val = vs[...]
        s = dot(qb, key, ((1,), (1,))) * scale
        e = jnp.exp(s - jnp.max(s, axis=-1, keepdims=True))
        prob = e * (1.0 / jnp.sum(e, axis=-1, keepdims=True))
        pb = prob.astype(BF16)
        out = dot(pb, val, ((1,), (0,))).astype(BF16).astype(F32)
        delta = jnp.sum(d.astype(F32) * out, axis=-1, keepdims=True)
        dp = dot(d, val, ((1,), (1,)))
        ds = (prob * (dp - delta) * scale).astype(BF16)
        dq = dot(ds, key, ((1,), (0,)))
        kp = dot(ds, qb, ((0,), (0,))).astype(BF16).astype(F32)
        vp = dot(pb, d, ((0,), (0,))).astype(BF16).astype(F32)
        if r == 0:
            dka[...] = kp
            dva[...] = vp
        else:
            dka[...] += kp
            dva[...] += vp
        dx, dg = norm_back(x, inv, gq, dq)
        dq_gain = dq_gain + dg
        outs[r][0:qn_rows] = dx.astype(BF16)
    for r in range(seq):
        x = parts[r][k0 : k0 + rows].astype(F32)
        dx, dg = norm_back(x, inverse_of(x), gk, dka[r * rows : (r + 1) * rows])
        dk_gain = dk_gain + dg
        outs[r][qn_rows : qn_rows + rows] = dx.astype(BF16)
        o = qn_rows + rows + trows
        outs[r][o : o + rows] = dva[r * rows : (r + 1) * rows].astype(BF16)
    dx, dg = norm_back(xt, inverse_of(xt), gk, dka[img : img + text])
    dk_gain = dk_gain + dg
    dka[img : img + text] = dx
    for r in range(seq):
        owner = lax.rem(pos_ref[0] + (seq - r), seq)
        at = pl.multiple_of(img + owner * trows, 16)
        o = qn_rows + rows
        outs[r][o : o + trows] = dka[pl.ds(at, trows)].astype(BF16)
        o = o + trows + rows
        outs[r][o : o + trows] = dva[pl.ds(at, trows)].astype(BF16)
    gout[0:1] = dq_gain
    gout[1:2] = dk_gain


def attend(pos, parts, text_k, text_v, q_gain, k_gain, gin, head, heads_here, rows, trows):
    seq = len(parts)
    keys = (rows + trows) * seq
    back = 3 * (rows + trows)

    def whole(shape):
        return pl.BlockSpec(shape, lambda i, p: (0,) * len(shape))

    tspec = pl.BlockSpec((text_k.shape[0], HEAD_DIM), lambda i, p: (0, p[0] * heads_here + head))
    return pl.pallas_call(
        functools.partial(attn_body, rows, trows, seq),
        grid_spec=pltpu.PrefetchScalarGridSpec(
            num_scalar_prefetch=1,
            grid=(1,),
            in_specs=[whole(p.shape) for p in parts]
            + [tspec, tspec, whole((1, HEAD_DIM)), whole((1, HEAD_DIM)), whole((2, HEAD_DIM))],
            out_specs=[whole((back, HEAD_DIM))] * seq + [whole((2, HEAD_DIM))],
            scratch_shapes=[
                pltpu.VMEM((keys, HEAD_DIM), BF16),
                pltpu.VMEM((keys, HEAD_DIM), BF16),
                pltpu.VMEM((keys, HEAD_DIM), F32),
                pltpu.VMEM((keys, HEAD_DIM), F32),
            ],
        ),
        out_shape=[jax.ShapeDtypeStruct((back, HEAD_DIM), BF16)] * seq
        + [jax.ShapeDtypeStruct((2, HEAD_DIM), F32)],
    )(pos, *parts, text_k, text_v, q_gain, k_gain, gin)


def unpack_body(rows, trows, seq, heads_here, pos_ref, *refs):
    n = seq * heads_here
    parts, outs = refs[:n], refs[n:]
    starts = (0, rows + trows, 2 * (rows + trows))
    for h in range(heads_here):
        for r in range(seq):
            p = parts[h * seq + r]
            col = (lax.rem(pos_ref[0] + r, seq) * heads_here + h) * HEAD_DIM
            lanes = pl.ds(pl.multiple_of(col, HEAD_DIM), HEAD_DIM)
            for j, at in enumerate(starts):
                outs[j][:, lanes] = p[at : at + rows]
                outs[3 + j][:, lanes] = p[at + rows : at + rows + trows]


def unpack(pos, parts, heads_here, seq, rows, trows):
    width = seq * heads_here * HEAD_DIM

    def whole(shape):
        return pl.BlockSpec(shape, lambda i, p: (0,) * len(shape))

    shapes = [(rows, width)] * 3 + [(trows, width)] * 3
    return pl.pallas_call(
        functools.partial(unpack_body, rows, trows, seq, heads_here),
        grid_spec=pltpu.PrefetchScalarGridSpec(
            num_scalar_prefetch=1,
            grid=(1,),
            in_specs=[whole(p.shape) for p in parts],
            out_specs=[whole(s) for s in shapes],
        ),
        out_shape=[jax.ShapeDtypeStruct(s, BF16) for s in shapes],
        name="unpack",
    )(pos, *parts)


def factors_of(n):
    found, f = [], 2
    while n > 1:
        while n % f == 0:
            found.append(f)
            n //= f
        f += 1
    return found


def sum_over(x, axis, factors):
    size = lax.axis_size(axis)
    index = lax.axis_index(axis)
    stride = 1
    for f in factors:
        digit = lax.rem(index // stride, f)

        def moved(i, k):
            dg = (i // stride) % f
            return i + ((dg + k) % f - dg) * stride

        got = [x]
        for k in range(1, f):
            got.append(lax.ppermute(x, axis, [(i, moved(i, k)) for i in range(size)]))
        if f == 2:
            x = got[0] + got[1]
        else:
            stack = jnp.stack(got)
            x = 0.0
            for j in range(f):
                x = x + lax.dynamic_index_in_dim(stack, lax.rem(digit - j + f, f), 0, False)
        stride *= f
    return x


def rotate(x, r, seq):
    return lax.ppermute(x, "seq", [(i, (i + r) % seq) for i in range(seq)])


def local(
    img_q_raw, img_k_raw, img_v, img_dout, txt_q_raw, txt_k_raw, txt_v, txt_dout, q_gain, k_gain
):
    seq = lax.axis_size("seq")
    pos = lax.axis_index("seq").astype(jnp.int32).reshape(1)
    rows, width = img_q_raw.shape[1:]
    trows = txt_q_raw.shape[1]
    heads_here = width // HEAD_DIM // seq
    arrays = (img_q_raw[0], txt_q_raw[0], img_dout[0], txt_dout[0], img_k_raw[0], img_v[0])
    text_k, text_v = txt_k_raw[0], txt_v[0]
    gq, gk = q_gain.reshape(1, HEAD_DIM), k_gain.reshape(1, HEAD_DIM)
    received = []
    for h in range(heads_here):
        sent = pack(pos, arrays, h, heads_here, seq)
        received.append([sent[0]] + [rotate(sent[r], r, seq) for r in range(1, seq)])
    gains = jnp.zeros((2, HEAD_DIM), F32)
    back = []
    for h in range(heads_here):
        *outs, gains = attend(
            pos, received[h], text_k, text_v, gq, gk, gains, h, heads_here, rows, trows
        )
        back.append([outs[0]] + [rotate(outs[r], seq - r, seq) for r in range(1, seq)])
    gains = sum_over(gains, "seq", [seq])
    gains = sum_over(gains, "dp", factors_of(lax.axis_size("dp")))
    flat = [part for parts in back for part in parts]
    grads = unpack(pos, flat, heads_here, seq, rows, trows)
    return tuple(g[None] for g in grads) + (gains[0], gains[1])


def solution(mesh):
    token = P("dp", "seq", None)
    shared = P("dp", None, None)
    return jax.shard_map(
        local,
        mesh=mesh,
        in_specs=(token, token, token, token, token, shared, shared, token, P(), P()),
        out_specs=(token,) * 6 + (P(), P()),
        check_vma=False,
    )
```
